32 devices in a mesh: band: 8 (over y, x, core), lev: 4 (over z).
Axes of the slice: x: 2, y: 2, z: 4, core: 2. Of those that a mesh axis runs over, the one named last changes fastest.
Arguments:
- pattern: float32 [1024, 128], P('band'), may hold values from -3 to 3
- taper: float32 [136], P('lev'), may hold values from 0.1 to 1
- thickness: float32 [136], P('lev'), may hold values from 0.2 to 2
- block_source: int32 [1024], P('band'), may hold values from 0 to 1023, as said below
- tendencies: bfloat16 [4, 136, 131072], P(None, 'lev', 'band'), may hold values from -6 to 6
Outputs:
- perturbed: bfloat16 [4, 136, 131072], P(None, 'lev', 'band')
- integrals: float32 [2, 131072], P(None, 'band')
The draws below stay inside these ranges and needn't reach their ends.
Inputs may be any that keep to these rules, and one draw needn't show every extreme that they name: block_source is a permutation of 0 to 1023; the 128 physics blocks of each band index take exactly 128 // 8 grid blocks from the 128 grid blocks of each band index.
All inputs are finite; a program needn't handle non-finite values.
Results may differ from the reference program's by a relative error of at most 0.001.
Values sent between devices are 32-bit elements; how exact they have to be, the bound alone decides.
A program may use at most 64 MiB of HBM per device.

```python
import math
import jax
import jax.numpy as jnp
from jax import lax

BLOCK = 128
LEV = 136
BLK_DEV = 128
NBLK = 1024
COLUMNS = 131072


def draw_block_source(key, part):
    bands = NBLK // BLK_DEV
    share = BLK_DEV // bands
    first_key, second_key = jax.random.split(jax.random.fold_in(key, 11))
    labels = jnp.repeat(jnp.arange(bands, dtype=jnp.int32), share)
    owner_keys = jax.random.split(first_key, bands)
    owners = jax.vmap(lambda k: jax.random.permutation(k, labels))(owner_keys).reshape(-1)
    grouped = jnp.argsort(owners, stable=True).astype(jnp.int32).reshape(bands, BLK_DEV)
    row_keys = jax.random.split(second_key, bands)
    shuffled = jax.vmap(lambda k, row: jax.random.permutation(k, row))(row_keys, grouped)
    return shuffled.reshape(-1).astype(jnp.int32)


def steps_of(stream_key, extent, pieces, low, top_value):
    gain, own = 1.0, jax.random.fold_in(stream_key, 6)
    for position, blocks in pieces:
        draws = jnp.exp(jax.random.uniform(jax.random.fold_in(own, position), (blocks,), jnp.float32, low / len(pieces), top_value / len(pieces)))
        gain = gain * jnp.repeat(draws, extent[position] // blocks).reshape([-1 if axis == position else 1 for axis in range(len(extent))])
    return gain


def gaussian(stream_key, extent, deviation, most, shards=(), kind=jnp.bfloat16):
    result = jax.random.normal(stream_key, extent, jnp.float32) * deviation
    if len(shards) > 0:
        result = steps_of(stream_key, extent, shards, -0.22, 0.18) * result
    return jnp.clip(result, min=-most, max=most).astype(kind)


def setup_inputs(seed: int = 0) -> dict:
    keys = jax.random.split(jax.random.key(seed), 6)
    return {
        "pattern": gaussian(keys[0], (NBLK, BLOCK), 0.6, 3.0, ((0, 8),), jnp.float32),
        "taper": jnp.clip(0.1 + 0.9 * jax.random.uniform(keys[1], (LEV,), jnp.float32) ** steps_of(keys[1], (LEV,), ((0, 4),), -0.2, 0.2), 0.1, 1.0),
        "thickness": jnp.clip(jnp.exp(math.log(2.0) - 2.3025851 * jax.random.uniform(keys[2], (LEV,), jnp.float32) ** steps_of(keys[2], (LEV,), ((0, 4),), -0.2, 0.2)), 0.2, 2.0),
        "block_source": draw_block_source(jax.random.fold_in(keys[5], 71), 0),
        "tendencies": gaussian(keys[4], (4, LEV, COLUMNS), 1.0, 6.0, ((1, 4), (2, 8))),
    }


def reference(pattern, taper, thickness, block_source, tendencies):
    clipped = jnp.tanh(pattern)
    local = jnp.take(clipped, block_source, axis=0).reshape(-1)
    pert = taper[:, None] * local[None, :]

    def scale_field(field):
        return (field.astype(jnp.float32) * (1.0 + pert)).astype(jnp.bfloat16)
    perturbed = lax.map(scale_field, tendencies)

    def column_sum(field):
        return lax.optimization_barrier(jnp.sum(thickness[:, None] * field.astype(jnp.float32) * pert, axis=0))
    norm_value = jnp.sqrt(jnp.sum(thickness * thickness))
    integrals = lax.map(column_sum, tendencies[2:4]) / norm_value
    return (perturbed, integrals)
```

```python
import functools
import jax
import jax.numpy as jnp
from jax import lax
from jax.experimental import pallas as pl
from jax.experimental.pallas import tpu as pltpu
from jax.sharding import PartitionSpec as P

MESH = pl.DeviceIdType.MESH


def exchange(n_band, n_lev, pattern, source_hbm, taper_hbm, thickness_hbm, tend, held, spread, totals,
             whole, acc, part, inbox, source, taper, thickness, small_sem, own_sem, load_sem, out_sem, in_sem, pass_sem, got_sem,
             part_send, part_recv, total_send, total_recv):
    band, lev = lax.axis_index("band"), lax.axis_index("lev")
    levels, rows, lanes = tend.shape
    blocks = pattern.shape[0]
    fields = rows // blocks
    share, piece = blocks // n_lev, rows // n_lev
    pairs = n_band // 2
    pair, core = band // 2, band % 2
    mate = pair * 2 + 1 - core

    def chunk_of(step):
        return lax.rem(lev + 1 + step, n_lev)

    def load(step):
        span = pl.ds(pl.multiple_of(chunk_of(step) * piece, piece), piece)
        return pltpu.make_async_copy(tend.at[:, span, :], held.at[:, span, :], load_sem.at[step])

    def block_rows(who):
        return pl.ds(pl.multiple_of(who * blocks, blocks), blocks)

    own = pltpu.make_async_copy(pattern, whole.at[block_rows(band)], own_sem)
    own.start()
    small = [pltpu.make_async_copy(a, b, small_sem.at[i]) for i, (a, b) in enumerate(
        ((thickness_hbm, thickness), (taper_hbm, taper), (source_hbm, source)))]
    for copy in small:
        copy.start()
    for step in range(n_lev):
        load(step).start()

    barrier = pltpu.get_barrier_semaphore()
    pl.semaphore_signal(barrier, inc=1, device_id={"band": mate}, device_id_type=MESH)
    for d in range(1, pairs):
        peer = lax.rem(pair + d, pairs) * 2 + core
        pl.semaphore_signal(barrier, inc=1, device_id={"band": peer}, device_id_type=MESH)
    for d in range(1, n_lev):
        pl.semaphore_signal(barrier, inc=1, device_id={"lev": lax.rem(lev + d, n_lev)}, device_id_type=MESH)
    own.wait()
    pl.semaphore_wait(barrier, pairs + n_lev - 1)

    def direct(d):
        peer = lax.rem(pair + d, pairs) * 2 + core
        mine = whole.at[block_rows(band)]
        return pltpu.make_async_remote_copy(mine, mine, out_sem.at[d], in_sem.at[d],
                                            device_id={"band": peer}, device_id_type=MESH)

    def relay(d):
        origin = lax.rem(pair - d + pairs, pairs) * 2 + core
        block = whole.at[block_rows(origin)]
        return pltpu.make_async_remote_copy(block, block, pass_sem.at[d], got_sem.at[d],
                                            device_id={"band": mate}, device_id_type=MESH)

    for d in range(1, pairs):
        direct(d).start()
    relay(0).start()

    for copy in small:
        copy.wait()
    squares = thickness[0] * thickness[0]
    for l in range(1, levels):
        squares += thickness[l] * thickness[l]

    def give(step):
        owner = chunk_of(step)
        return pltpu.make_async_remote_copy(part.at[step], inbox.at[n_lev - 2 - step], part_send.at[step],
                                            part_recv.at[n_lev - 2 - step],
                                            device_id={"lev": owner}, device_id_type=MESH)

    for step in range(n_lev):
        load(step).wait()
        first = pl.multiple_of(chunk_of(step) * piece, piece)
        for r in range(0, piece, 64):
            def add(l, total):
                weight = thickness[l] * taper[l]
                return total + weight * held[l, pl.ds(first + r, 64), :].astype(jnp.float32)
            acc[pl.ds(r, 64), :] = lax.fori_loop(0, levels, add, jnp.zeros((64, lanes), jnp.float32), unroll=2)
        for k in range(2):
            part[step, k * share:(k + 1) * share, :] = acc[pl.ds(fields - 2 + k, share, stride=fields), :]
        part[step, 2 * share:, :] = jnp.full((8, lanes), squares, jnp.float32)
        if step < n_lev - 1:
            give(step).start()

    def arrived(d):
        direct(d).wait_recv()
        relay(d).start()

    for d in range(1, pairs):
        arrived(d)

    for step in range(n_lev - 1):
        give(step).wait()
    total = part[n_lev - 1]
    for slot in range(n_lev - 1):
        total = total + inbox[slot]
    totals[lev] = total[:2 * share] / jnp.sqrt(total[2 * share:2 * share + 1])

    def publish(d):
        return pltpu.make_async_remote_copy(totals.at[lev], totals.at[lev], total_send.at[d], total_recv.at[d],
                                            device_id={"lev": lax.rem(lev + d, n_lev)}, device_id_type=MESH)

    for d in range(1, n_lev):
        publish(d).start()

    for d in range(pairs):
        relay(d).wait()
    for d in range(1, pairs):
        direct(d).wait_send()

    def pick(j, _):
        row = whole[pl.ds(source[j], 1), :]
        acc[pl.ds(j, 1), :] = row
        return 0

    lax.fori_loop(0, blocks, pick, 0, unroll=8)
    local = jnp.tanh(acc[0:blocks, :])
    for f in range(fields):
        spread[pl.ds(f, blocks, stride=fields), :] = local

    for d in range(1, n_lev):
        publish(d).wait()


def scale(n_lev, taper, held, spread, totals, out, column, made, sums, out_sem, sum_sem):
    levels, rows, lanes = held.shape
    blocks = column.shape[0]
    share, fields = blocks // n_lev, rows // blocks

    def level(l, _):
        for r in range(0, rows, 64):
            factor = 1.0 + taper[l] * spread[pl.ds(r, 64), :]
            made[l, pl.ds(r, 64), :] = (held[l, pl.ds(r, 64), :].astype(jnp.float32) * factor).astype(made.dtype)
        pltpu.make_async_copy(made.at[l], out.at[l], out_sem.at[l]).start()
        return 0

    lax.fori_loop(0, levels, level, 0)
    for c in range(n_lev):
        local = spread[pl.ds(c * share * fields, share, stride=fields), :]
        for k in range(2):
            sums[c * share:(c + 1) * share, k, :] = totals[c, k * share:(k + 1) * share, :] * local
    done = pltpu.make_async_copy(sums, column, sum_sem)
    done.start()

    def finish(l, _):
        pltpu.make_async_copy(made.at[l], out.at[l], out_sem.at[l]).wait()
        return 0

    lax.fori_loop(0, levels, finish, 0)
    done.wait()


def body(n_band, n_lev, pattern, taper, thickness, block_source, tendencies):
    fields, levels, columns = tendencies.shape
    blocks, lanes = pattern.shape
    rows = blocks * fields
    share, piece, pairs = blocks // n_lev, rows // n_lev, n_band // 2
    tend = tendencies.transpose(1, 0, 2).reshape(levels, fields, blocks, lanes)
    tend = tend.transpose(0, 2, 1, 3).reshape(levels, rows, lanes)
    anywhere = pl.BlockSpec(memory_space=pl.ANY)
    hbm = pl.BlockSpec(memory_space=pltpu.HBM)
    scalars = pl.BlockSpec(memory_space=pltpu.SMEM)
    vector = pl.BlockSpec(memory_space=pltpu.VMEM)
    f32, dma = jnp.float32, pltpu.SemaphoreType.DMA
    held, spread, totals = pl.pallas_call(
        functools.partial(exchange, n_band, n_lev),
        name="exchange",
        out_shape=(pltpu.VMEM(tend.shape, tend.dtype), pltpu.VMEM((rows, lanes), f32),
                   pltpu.VMEM((n_lev, 2 * share, lanes), f32)),
        in_specs=[hbm] * 5,
        out_specs=(vector, vector, vector),
        scratch_shapes=[
            pltpu.VMEM((n_band * blocks, lanes), f32),
            pltpu.VMEM((max(piece, blocks), lanes), f32),
            pltpu.VMEM((n_lev, 2 * share + 8, lanes), f32),
            pltpu.VMEM((n_lev - 1, 2 * share + 8, lanes), f32),
            pltpu.SMEM(block_source.shape, jnp.int32), pltpu.SMEM(taper.shape, f32),
            pltpu.SMEM(thickness.shape, f32), dma((3,)),
            dma, dma((n_lev,)), dma((pairs,)), dma((pairs,)), dma((pairs,)), dma((pairs,)),
            dma((n_lev,)), dma((n_lev,)), dma((n_lev,)), dma((n_lev,)),
        ],
        compiler_params=pltpu.CompilerParams(collective_id=0, has_side_effects=True, vmem_limit_bytes=12 << 20),
    )(*(pltpu.with_memory_space_constraint(x, pltpu.MemorySpace.HBM)
        for x in (pattern, block_source, taper, thickness, tend)))
    in_vmem = lambda x: pltpu.with_memory_space_constraint(x, pltpu.MemorySpace.VMEM)
    out, column = pl.pallas_call(
        functools.partial(scale, n_lev),
        name="scale",
        out_shape=(jax.ShapeDtypeStruct(tend.shape, tend.dtype), jax.ShapeDtypeStruct((blocks, 2, lanes), f32)),
        in_specs=[scalars, vector, vector, vector],
        out_specs=(anywhere, anywhere),
        scratch_shapes=[pltpu.VMEM(tend.shape, tend.dtype), pltpu.VMEM((blocks, 2, lanes), f32), dma((levels,)), dma],
        compiler_params=pltpu.CompilerParams(vmem_limit_bytes=24 << 20),
    )(taper, in_vmem(held), in_vmem(spread), in_vmem(totals))
    out = out.reshape(levels, blocks, fields, lanes).transpose(2, 0, 1, 3).reshape(fields, levels, columns)
    return out, column.transpose(1, 0, 2).reshape(2, columns)


def solution(mesh):
    in_specs = (P("band", None), P("lev"), P("lev"), P("band"), P(None, "lev", "band"))
    out_specs = (P(None, "lev", "band"), P(None, "band"))
    run = functools.partial(body, mesh.shape["band"], mesh.shape["lev"])
    return jax.shard_map(run, mesh=mesh, in_specs=in_specs, out_specs=out_specs, check_vma=False)
```

```python
import functools
import jax
import jax.numpy as jnp
from jax import lax
from jax.experimental import pallas as pl
from jax.experimental.pallas import tpu as pltpu
from jax.sharding import PartitionSpec as P

MESH = pl.DeviceIdType.MESH


def exchange(n_band, n_lev, pattern, source_hbm, taper_hbm, thickness_hbm, tend, held, spread, totals,
             whole, acc, part, inbox, source, taper, thickness, small_sem, own_sem, load_sem, out_sem, in_sem, pass_sem, got_sem,
             part_send, part_recv, total_send, total_recv):
    band, lev = lax.axis_index("band"), lax.axis_index("lev")
    levels, rows, lanes = tend.shape
    blocks = pattern.shape[0]
    fields = rows // blocks
    pieces, half = totals.shape[0], n_lev // 2
    share, piece = blocks // pieces, rows // pieces
    pairs = n_band // 2
    per = pieces // 2
    side = lev // half
    near, far = half - 1 + side, half - side
    pair, core = band // 2, band % 2
    mate = pair * 2 + 1 - core

    def chunk_of(step):
        return lax.rem(step + (1 - side) * per, pieces)

    def load(step):
        span = pl.ds(pl.multiple_of(chunk_of(step) * piece, piece), piece)
        return pltpu.make_async_copy(tend.at[:, span, :], held.at[:, span, :], load_sem.at[step])

    def block_rows(who):
        return pl.ds(pl.multiple_of(who * blocks, blocks), blocks)

    own = pltpu.make_async_copy(pattern, whole.at[block_rows(band)], own_sem)
    own.start()
    small = [pltpu.make_async_copy(a, b, small_sem.at[i]) for i, (a, b) in enumerate(
        ((thickness_hbm, thickness), (taper_hbm, taper), (source_hbm, source)))]
    for copy in small:
        copy.start()
    for step in range(pieces):
        load(step).start()

    barrier = pltpu.get_barrier_semaphore()
    pl.semaphore_signal(barrier, inc=1, device_id={"band": mate}, device_id_type=MESH)
    for d in range(1, pairs):
        peer = lax.rem(pair + d, pairs) * 2 + core
        pl.semaphore_signal(barrier, inc=1, device_id={"band": peer}, device_id_type=MESH)
    for d in range(1, n_lev):
        peer = lax.rem(lev + d, n_lev)

        @pl.when((lev == near) | (peer == half - 1) | (peer == half))
        def _(peer=peer):
            pl.semaphore_signal(barrier, inc=1, device_id={"lev": peer}, device_id_type=MESH)

    def direct(d):
        peer = lax.rem(pair + d, pairs) * 2 + core
        mine = whole.at[block_rows(band)]
        return pltpu.make_async_remote_copy(mine, mine, out_sem.at[d], in_sem.at[d],
                                            device_id={"band": peer}, device_id_type=MESH)

    def relay(d):
        origin = lax.rem(pair - d + pairs, pairs) * 2 + core
        block = whole.at[block_rows(origin)]
        return pltpu.make_async_remote_copy(block, block, pass_sem.at[d], got_sem.at[d],
                                            device_id={"band": mate}, device_id_type=MESH)

    for copy in small:
        copy.wait()
    squares = thickness[0] * thickness[0]
    for l in range(1, levels):
        squares += thickness[l] * thickness[l]

    def give(step):
        return pltpu.make_async_remote_copy(part.at[step], inbox.at[lev, step % per], part_send.at[step],
                                            part_recv.at[lev, step % per],
                                            device_id={"lev": far if step < per else near}, device_id_type=MESH)

    def got(peer, q):
        return pltpu.make_async_remote_copy(part.at[q], inbox.at[peer, q], part_send.at[q], part_recv.at[peer, q],
                                            device_id={"lev": peer}, device_id_type=MESH)

    def publish(d, q):
        mine = totals.at[side * per + q]
        return pltpu.make_async_remote_copy(mine, mine, total_send.at[d, q], total_recv.at[side * per + q],
                                            device_id={"lev": lax.rem(lev + d, n_lev)}, device_id_type=MESH)

    def send(step):
        if step < per:
            give(step).start()
        else:
            pl.when(lev != near)(lambda: give(step).start())

    def level_sums(step):
        load(step).wait()
        first = pl.multiple_of(chunk_of(step) * piece, piece)
        for r in range(0, piece, 64):
            def add(l, total):
                weight = thickness[l] * taper[l]
                return total + weight * held[l, pl.ds(first + r, 64), :].astype(jnp.float32)
            acc[pl.ds(r, 64), :] = lax.fori_loop(0, levels, add, jnp.zeros((64, lanes), jnp.float32), unroll=34)
        for k in range(2):
            part[step, k * share:(k + 1) * share, :] = acc[pl.ds(fields - 2 + k, share, stride=fields), :]
        part[step, 2 * share:, :] = jnp.full((8, lanes), squares, jnp.float32)

    for step in range(2):
        level_sums(step)
    own.wait()
    met = jnp.where(lev == near, n_lev - 1, 2)
    pl.semaphore_wait(barrier, pairs + met)
    for step in range(2):
        send(step)
    for d in range(1, pairs):
        direct(d).start()
    relay(0).start()

    for step in range(2, pieces):
        level_sums(step)
        send(step)

    @pl.when(lev == near)
    def _():
        for q in range(per):
            total = part[per + q]
            for d in range(1, n_lev):
                peer = lax.rem(lev + d, n_lev)
                got(peer, q).wait_recv()
                total = total + inbox[peer, q]
            totals[side * per + q] = total[:2 * share] / jnp.sqrt(total[2 * share:2 * share + 1])
            for d in range(1, n_lev):
                publish(d, q).start()

    for d in range(1, pairs):
        direct(d).wait_recv()
        relay(d).start()
    for d in range(pairs):
        relay(d).wait()
    for d in range(1, pairs):
        direct(d).wait_send()

    def pick(j, _):
        row = whole[pl.ds(source[j], 1), :]
        acc[pl.ds(j, 1), :] = row
        return 0

    lax.fori_loop(0, blocks, pick, 0, unroll=32)
    local = jnp.tanh(acc[0:blocks, :])
    for f in range(fields):
        spread[pl.ds(f, blocks, stride=fields), :] = local

    for step in range(pieces):
        if step < per:
            give(step).wait_send()
        else:
            pl.when(lev != near)(lambda step=step: give(step).wait_send())

    @pl.when(lev == near)
    def _():
        for q in range(per):
            for d in range(1, n_lev):
                publish(d, q).wait_send()

    for p in range(pieces):
        @pl.when(lev != half - 1 + p // per)
        def _(p=p):
            pltpu.make_async_remote_copy(totals.at[p], totals.at[p], total_send.at[0, 0], total_recv.at[p],
                                         device_id={"lev": far}, device_id_type=MESH).wait_recv()


def scale(taper, held, spread, totals, out, column, made, sums, out_sem, sum_sem):
    levels, rows, lanes = held.shape
    blocks = column.shape[0]
    pieces = totals.shape[0]
    share, fields = blocks // pieces, rows // blocks

    def level(l, _):
        for r in range(0, rows, 64):
            factor = 1.0 + taper[l] * spread[pl.ds(r, 64), :]
            made[l, pl.ds(r, 64), :] = (held[l, pl.ds(r, 64), :].astype(jnp.float32) * factor).astype(made.dtype)
        pltpu.make_async_copy(made.at[l], out.at[l], out_sem.at[l]).start()
        return 0

    lax.fori_loop(0, levels, level, 0)
    for c in range(pieces):
        local = spread[pl.ds(c * share * fields, share, stride=fields), :]
        for k in range(2):
            sums[c * share:(c + 1) * share, k, :] = totals[c, k * share:(k + 1) * share, :] * local
    done = pltpu.make_async_copy(sums, column, sum_sem)
    done.start()

    def finish(l, _):
        pltpu.make_async_copy(made.at[l], out.at[l], out_sem.at[l]).wait()
        return 0

    lax.fori_loop(0, levels, finish, 0)
    done.wait()


def body(n_band, n_lev, pattern, taper, thickness, block_source, tendencies):
    fields, levels, columns = tendencies.shape
    blocks, lanes = pattern.shape
    rows = blocks * fields
    pieces = 4
    share, piece, pairs = blocks // pieces, rows // pieces, n_band // 2
    tend = tendencies.transpose(1, 0, 2).reshape(levels, fields, blocks, lanes)
    tend = tend.transpose(0, 2, 1, 3).reshape(levels, rows, lanes)
    anywhere = pl.BlockSpec(memory_space=pl.ANY)
    hbm = pl.BlockSpec(memory_space=pltpu.HBM)
    scalars = pl.BlockSpec(memory_space=pltpu.SMEM)
    vector = pl.BlockSpec(memory_space=pltpu.VMEM)
    f32, dma = jnp.float32, pltpu.SemaphoreType.DMA
    held, spread, totals = pl.pallas_call(
        functools.partial(exchange, n_band, n_lev),
        name="exchange",
        out_shape=(pltpu.VMEM(tend.shape, tend.dtype), pltpu.VMEM((rows, lanes), f32),
                   pltpu.VMEM((pieces, 2 * share, lanes), f32)),
        in_specs=[hbm] * 5,
        out_specs=(vector, vector, vector),
        scratch_shapes=[
            pltpu.VMEM((n_band * blocks, lanes), f32),
            pltpu.VMEM((max(piece, blocks), lanes), f32),
            pltpu.VMEM((pieces, 2 * share + 8, lanes), f32),
            pltpu.VMEM((n_lev, pieces // 2, 2 * share + 8, lanes), f32),
            pltpu.SMEM(block_source.shape, jnp.int32), pltpu.SMEM(taper.shape, f32),
            pltpu.SMEM(thickness.shape, f32), dma((3,)),
            dma, dma((pieces,)), dma((pairs,)), dma((pairs,)), dma((pairs,)), dma((pairs,)),
            dma((pieces,)), dma((n_lev, pieces // 2)), dma((n_lev, pieces // 2)), dma((pieces,)),
        ],
        compiler_params=pltpu.CompilerParams(collective_id=0, has_side_effects=True, vmem_limit_bytes=12 << 20),
    )(*(pltpu.with_memory_space_constraint(x, pltpu.MemorySpace.HBM)
        for x in (pattern, block_source, taper, thickness, tend)))
    in_vmem = lambda x: pltpu.with_memory_space_constraint(x, pltpu.MemorySpace.VMEM)
    out, column = pl.pallas_call(
        scale,
        name="scale",
        out_shape=(jax.ShapeDtypeStruct(tend.shape, tend.dtype), jax.ShapeDtypeStruct((blocks, 2, lanes), f32)),
        in_specs=[scalars, vector, vector, vector],
        out_specs=(anywhere, anywhere),
        scratch_shapes=[pltpu.VMEM(tend.shape, tend.dtype), pltpu.VMEM((blocks, 2, lanes), f32), dma((levels,)), dma],
        compiler_params=pltpu.CompilerParams(vmem_limit_bytes=24 << 20),
    )(taper, in_vmem(held), in_vmem(spread), in_vmem(totals))
    out = out.reshape(levels, blocks, fields, lanes).transpose(2, 0, 1, 3).reshape(fields, levels, columns)
    return out, column.transpose(1, 0, 2).reshape(2, columns)


def solution(mesh):
    in_specs = (P("band", None), P("lev"), P("lev"), P("band"), P(None, "lev", "band"))
    out_specs = (P(None, "lev", "band"), P(None, "band"))
    run = functools.partial(body, mesh.shape["band"], mesh.shape["lev"])
    return jax.shard_map(run, mesh=mesh, in_specs=in_specs, out_specs=out_specs, check_vma=False)
```

```python
import functools
import jax
import jax.numpy as jnp
from jax import lax
from jax.experimental import pallas as pl
from jax.experimental.pallas import tpu as pltpu
from jax.sharding import PartitionSpec as P

MESH = pl.DeviceIdType.MESH


def exchange(n_band, n_lev, pattern, source_hbm, taper_hbm, thickness_hbm, tend, held, spread, totals,
             whole, acc, part, inbox, source, taper, thickness, small_sem, own_sem, load_sem, out_sem, in_sem, pass_sem, got_sem,
             part_send, part_recv, total_send, total_recv):
    band, lev = lax.axis_index("band"), lax.axis_index("lev")
    levels, rows, lanes = tend.shape
    blocks = pattern.shape[0]
    fields = rows // blocks
    pieces, half = totals.shape[0], n_lev // 2
    share, piece = blocks // pieces, rows // pieces
    pairs = n_band // 2
    per = pieces // 2
    side = lev // half
    near, far = half - 1 + side, half - side
    pair, core = band // 2, band % 2
    mate = pair * 2 + 1 - core

    def chunk_of(step):
        owner = 1 - side if step % 2 == 0 else side
        return owner * per + step // 2

    def load(step):
        span = pl.ds(pl.multiple_of(chunk_of(step) * piece, piece), piece)
        return pltpu.make_async_copy(tend.at[:, span, :], held.at[:, span, :], load_sem.at[step])

    def block_rows(who):
        return pl.ds(pl.multiple_of(who * blocks, blocks), blocks)

    own = pltpu.make_async_copy(pattern, whole.at[block_rows(band)], own_sem)
    own.start()
    small = [pltpu.make_async_copy(a, b, small_sem.at[i]) for i, (a, b) in enumerate(
        ((thickness_hbm, thickness), (taper_hbm, taper), (source_hbm, source)))]
    for copy in small:
        copy.start()
    for step in range(pieces):
        load(step).start()

    barrier = pltpu.get_barrier_semaphore()
    pl.semaphore_signal(barrier, inc=1, device_id={"band": mate}, device_id_type=MESH)
    for d in range(1, pairs):
        peer = lax.rem(pair + d, pairs) * 2 + core
        pl.semaphore_signal(barrier, inc=1, device_id={"band": peer}, device_id_type=MESH)
    for d in range(1, n_lev):
        peer = lax.rem(lev + d, n_lev)

        @pl.when((lev == near) | (peer == half - 1) | (peer == half))
        def _(peer=peer):
            pl.semaphore_signal(barrier, inc=1, device_id={"lev": peer}, device_id_type=MESH)

    def direct(d):
        peer = lax.rem(pair + d, pairs) * 2 + core
        mine = whole.at[block_rows(band)]
        return pltpu.make_async_remote_copy(mine, mine, out_sem.at[d], in_sem.at[d],
                                            device_id={"band": peer}, device_id_type=MESH)

    def relay(d):
        origin = lax.rem(pair - d + pairs, pairs) * 2 + core
        block = whole.at[block_rows(origin)]
        return pltpu.make_async_remote_copy(block, block, pass_sem.at[d], got_sem.at[d],
                                            device_id={"band": mate}, device_id_type=MESH)

    for copy in small:
        copy.wait()
    squares = thickness[0] * thickness[0]
    for l in range(1, levels):
        squares += thickness[l] * thickness[l]

    def give(step):
        return pltpu.make_async_remote_copy(part.at[step], inbox.at[lev, step // 2], part_send.at[step],
                                            part_recv.at[lev, step // 2],
                                            device_id={"lev": far if step % 2 == 0 else near}, device_id_type=MESH)

    def got(peer, q):
        return pltpu.make_async_remote_copy(part.at[q], inbox.at[peer, q], part_send.at[q], part_recv.at[peer, q],
                                            device_id={"lev": peer}, device_id_type=MESH)

    def publish(d, q):
        mine = totals.at[side * per + q]
        return pltpu.make_async_remote_copy(mine, mine, total_send.at[d, q], total_recv.at[side * per + q],
                                            device_id={"lev": lax.rem(lev + d, n_lev)}, device_id_type=MESH)

    def send(step):
        if step % 2 == 0:
            give(step).start()
        else:
            pl.when(lev != near)(lambda: give(step).start())

    def level_sums(step):
        load(step).wait()
        first = pl.multiple_of(chunk_of(step) * piece, piece)
        for r in range(0, piece, 64):
            def add(l, total):
                weight = thickness[l] * taper[l]
                return total + weight * held[l, pl.ds(first + r, 64), :].astype(jnp.float32)
            acc[pl.ds(r, 64), :] = lax.fori_loop(0, levels, add, jnp.zeros((64, lanes), jnp.float32), unroll=34)
        for k in range(2):
            part[step, k * share:(k + 1) * share, :] = acc[pl.ds(fields - 2 + k, share, stride=fields), :]
        part[step, 2 * share:, :] = jnp.full((1, lanes), squares, jnp.float32)

    for step in range(2):
        level_sums(step)
    own.wait()
    met = jnp.where(lev == near, n_lev - 1, 2)
    pl.semaphore_wait(barrier, pairs + met)
    for step in range(2):
        send(step)
    for d in range(1, pairs):
        direct(d).start()
    relay(0).start()

    for step in range(2, pieces):
        level_sums(step)
        send(step)

    @pl.when(lev == near)
    def _():
        for q in range(per):
            total = part[2 * q + 1]
            for d in range(1, n_lev):
                peer = lax.rem(lev + d, n_lev)
                got(peer, q).wait_recv()
                total = total + inbox[peer, q]
            totals[side * per + q] = total[:2 * share] / jnp.sqrt(total[2 * share:2 * share + 1])
            for d in range(1, n_lev):
                publish(d, q).start()

    for d in range(1, pairs):
        direct(d).wait_recv()
        relay(d).start()
    for d in range(pairs):
        relay(d).wait()
    for d in range(1, pairs):
        direct(d).wait_send()

    def pick(j, _):
        row = whole[pl.ds(source[j], 1), :]
        acc[pl.ds(j, 1), :] = row
        return 0

    lax.fori_loop(0, blocks, pick, 0, unroll=32)
    local = jnp.tanh(acc[0:blocks, :])
    for f in range(fields):
        spread[pl.ds(f, blocks, stride=fields), :] = local

    for step in range(pieces):
        if step % 2 == 0:
            give(step).wait_send()
        else:
            pl.when(lev != near)(lambda step=step: give(step).wait_send())

    @pl.when(lev == near)
    def _():
        for q in range(per):
            for d in range(1, n_lev):
                publish(d, q).wait_send()

    for p in range(pieces):
        @pl.when(lev != half - 1 + p // per)
        def _(p=p):
            pltpu.make_async_remote_copy(totals.at[p], totals.at[p], total_send.at[0, 0], total_recv.at[p],
                                         device_id={"lev": far}, device_id_type=MESH).wait_recv()


def scale(taper, held, spread, totals, out, column, made, sums, out_sem, sum_sem):
    levels, rows, lanes = held.shape
    blocks = column.shape[0]
    pieces = totals.shape[0]
    share, fields = blocks // pieces, rows // blocks

    def level(l, _):
        for r in range(0, rows, 64):
            factor = 1.0 + taper[l] * spread[pl.ds(r, 64), :]
            made[l, pl.ds(r, 64), :] = (held[l, pl.ds(r, 64), :].astype(jnp.float32) * factor).astype(made.dtype)
        pltpu.make_async_copy(made.at[l], out.at[l], out_sem.at[l]).start()
        return 0

    lax.fori_loop(0, levels, level, 0)
    for c in range(pieces):
        local = spread[pl.ds(c * share * fields, share, stride=fields), :]
        for k in range(2):
            sums[c * share:(c + 1) * share, k, :] = totals[c, k * share:(k + 1) * share, :] * local
    done = pltpu.make_async_copy(sums, column, sum_sem)
    done.start()

    def finish(l, _):
        pltpu.make_async_copy(made.at[l], out.at[l], out_sem.at[l]).wait()
        return 0

    lax.fori_loop(0, levels, finish, 0)
    done.wait()


def body(n_band, n_lev, pattern, taper, thickness, block_source, tendencies):
    fields, levels, columns = tendencies.shape
    blocks, lanes = pattern.shape
    rows = blocks * fields
    pieces = 4
    share, piece, pairs = blocks // pieces, rows // pieces, n_band // 2
    tend = tendencies.transpose(1, 0, 2).reshape(levels, fields, blocks, lanes)
    tend = tend.transpose(0, 2, 1, 3).reshape(levels, rows, lanes)
    anywhere = pl.BlockSpec(memory_space=pl.ANY)
    hbm = pl.BlockSpec(memory_space=pltpu.HBM)
    scalars = pl.BlockSpec(memory_space=pltpu.SMEM)
    vector = pl.BlockSpec(memory_space=pltpu.VMEM)
    f32, dma = jnp.float32, pltpu.SemaphoreType.DMA
    held, spread, totals = pl.pallas_call(
        functools.partial(exchange, n_band, n_lev),
        name="exchange",
        out_shape=(pltpu.VMEM(tend.shape, tend.dtype), pltpu.VMEM((rows, lanes), f32),
                   pltpu.VMEM((pieces, 2 * share, lanes), f32)),
        in_specs=[hbm] * 5,
        out_specs=(vector, vector, vector),
        scratch_shapes=[
            pltpu.VMEM((n_band * blocks, lanes), f32),
            pltpu.VMEM((max(piece, blocks), lanes), f32),
            pltpu.VMEM((pieces, 2 * share + 1, lanes), f32),
            pltpu.VMEM((n_lev, pieces // 2, 2 * share + 1, lanes), f32),
            pltpu.SMEM(block_source.shape, jnp.int32), pltpu.SMEM(taper.shape, f32),
            pltpu.SMEM(thickness.shape, f32), dma((3,)),
            dma, dma((pieces,)), dma((pairs,)), dma((pairs,)), dma((pairs,)), dma((pairs,)),
            dma((pieces,)), dma((n_lev, pieces // 2)), dma((n_lev, pieces // 2)), dma((pieces,)),
        ],
        compiler_params=pltpu.CompilerParams(collective_id=0, has_side_effects=True, vmem_limit_bytes=12 << 20),
    )(*(pltpu.with_memory_space_constraint(x, pltpu.MemorySpace.HBM)
        for x in (pattern, block_source, taper, thickness, tend)))
    in_vmem = lambda x: pltpu.with_memory_space_constraint(x, pltpu.MemorySpace.VMEM)
    out, column = pl.pallas_call(
        scale,
        name="scale",
        out_shape=(jax.ShapeDtypeStruct(tend.shape, tend.dtype), jax.ShapeDtypeStruct((blocks, 2, lanes), f32)),
        in_specs=[scalars, vector, vector, vector],
        out_specs=(anywhere, anywhere),
        scratch_shapes=[pltpu.VMEM(tend.shape, tend.dtype), pltpu.VMEM((blocks, 2, lanes), f32), dma((levels,)), dma],
        compiler_params=pltpu.CompilerParams(vmem_limit_bytes=24 << 20),
    )(taper, in_vmem(held), in_vmem(spread), in_vmem(totals))
    out = out.reshape(levels, blocks, fields, lanes).transpose(2, 0, 1, 3).reshape(fields, levels, columns)
    return out, column.transpose(1, 0, 2).reshape(2, columns)


def solution(mesh):
    in_specs = (P("band", None), P("lev"), P("lev"), P("band"), P(None, "lev", "band"))
    out_specs = (P(None, "lev", "band"), P(None, "band"))
    run = functools.partial(body, mesh.shape["band"], mesh.shape["lev"])
    return jax.shard_map(run, mesh=mesh, in_specs=in_specs, out_specs=out_specs, check_vma=False)
```
